32 devices in a mesh: node: 8 (over y, x, core), chip: 4 (over z).
Axes of the slice: x: 2, y: 2, z: 4, core: 2. Of those that a mesh axis runs over, the one named last changes fastest.
Arguments:
- momentum: float32 [32, 128, 512], P(('node', 'chip')), may hold values from -6 to 6
- gradient: bfloat16 [32, 128, 512], P(('node', 'chip')), may hold values from -6 to 6
- indices: int32 [32, 16, 32], P(('node', 'chip')), may hold values from 0 to 4095, as said below
Outputs:
- new_momentum: float32 [32, 128, 512], P(('node', 'chip'))
- update: float32 [128, 512], replicated
The draws below stay inside these ranges and needn't reach their ends.
Inputs may be any that keep to these rules, and one draw needn't show every extreme that they name: `indices`: the 32 entries of each row name distinct coefficients of their span, coefficient (k, l) being k * 64 + l.
All inputs are finite; a program needn't handle non-finite values.
Results may differ from the reference program's by a relative error of at most 0.0029.
Values may be sent and summed in bfloat16 or wider, within the bound.
A program may use at most 64 MiB of HBM per device.

```python
import math
import jax
import jax.numpy as jnp
from jax import lax

KV_WIDTH = 512
ROWS = 128
SPAN = 64
TOPK = 32
SPANS = 16
REPL = 32


def draw_indices(key, part):
    seeds = jax.random.split(key, REPL)

    def draw_one(subkey):
        scores = jax.random.randint(subkey, (SPANS, SPAN * SPAN), 0, 2 ** 18) * (SPAN * SPAN)
        scores = scores + jnp.arange(SPAN * SPAN, dtype=jnp.int32)[None, :]
        unused, picked = lax.top_k(scores, TOPK)
        return picked.astype(jnp.int32)
    return lax.map(draw_one, seeds)


def level_of(own_key, dims, pieces, low, high):
    def one(dim, parts):
        steps = jax.random.uniform(jax.random.fold_in(jax.random.fold_in(own_key, 6), dim), (parts,), jnp.float32, low / len(pieces), high / len(pieces))
        return jnp.repeat(jnp.exp(steps), dims[dim] // parts).reshape((-1,) + (1,) * (len(dims) - dim - 1))

    gain = one(*pieces[0])
    for cut in pieces[1:]:
        gain = gain * one(*cut)
    return gain


def normal_values(rng, shape, spread, reach, pieces=(), held_as=jnp.bfloat16):
    array = jax.random.normal(rng, shape, jnp.float32) * spread
    if len(pieces) > 0:
        array = level_of(rng, shape, pieces, -0.22, 0.18) * array
    return jnp.clip(array, min=-reach, max=reach).astype(held_as)


def setup_inputs(seed: int = 0) -> dict:
    key_list = jax.random.split(jax.random.key(seed), 4)
    return {
        "momentum": normal_values(key_list[0], (REPL, ROWS, KV_WIDTH), 1.0, 6.0, ((0, 32),), jnp.float32),
        "gradient": normal_values(key_list[1], (REPL, ROWS, KV_WIDTH), 1.0, 6.0, ((0, 32),)),
        "indices": draw_indices(jax.random.fold_in(key_list[3], 71), 0),
    }


def dct_table(edge_len):
    orders = jnp.arange(edge_len, dtype=jnp.float32)
    wave_no = orders[:, None]
    cell_no = orders[None, :]
    factor = jnp.where(wave_no == 0.0, math.sqrt(1.0 / edge_len), math.sqrt(2.0 / edge_len))
    return factor * jnp.cos(math.pi * (2.0 * cell_no + 1.0) * wave_no / (2.0 * edge_len))

def forward(grid_field, cosines, edge_len):
    row_blocks = grid_field.shape[0] // edge_len
    col_blocks = grid_field.shape[1] // edge_len
    blocks = grid_field.reshape(row_blocks, edge_len, col_blocks, edge_len).transpose(0, 2, 1, 3)
    coeffs = jnp.einsum('kn,abnm,lm->abkl', cosines, blocks, cosines, precision=lax.Precision.HIGHEST)
    return coeffs.reshape(row_blocks * col_blocks, edge_len * edge_len)

def inverse_blocks(coeffs, cosines, edge_len):
    blocks = coeffs.reshape(coeffs.shape[0], edge_len, edge_len)
    return jnp.einsum('kn,ckl,lm->cnm', cosines, blocks, cosines, precision=lax.Precision.HIGHEST)

def place_blocks(blocks, row_count, col_count, edge_len):
    shaped = blocks.reshape(row_count // edge_len, col_count // edge_len, edge_len, edge_len)
    return shaped.transpose(0, 2, 1, 3).reshape(row_count, col_count)

def normalized(blocks):
    energy = lax.optimization_barrier(jnp.mean(blocks * blocks, axis=(1, 2), keepdims=True))
    return blocks / jnp.sqrt(energy + 1.0)

def add_entries(totals, picked, slots):
    span_ids = jnp.broadcast_to(jnp.arange(slots.shape[-2], dtype=jnp.int32)[:, None], slots.shape)
    return totals.at[span_ids, slots].add(picked.astype(jnp.float32))

def reference(momentum, gradient, indices):
    cosines = dct_table(SPAN)
    n_spans = ROWS // SPAN * (KV_WIDTH // SPAN)

    def replica_step(totals, inputs_row):
        moment, grad_row, slots = inputs_row
        blended = 0.9 * moment + grad_row.astype(jnp.float32)
        coeffs = forward(blended, cosines, SPAN)
        picked = jnp.take_along_axis(coeffs, slots, axis=1).astype(jnp.bfloat16)
        sparse = add_entries(jnp.zeros_like(coeffs), picked, slots)
        own_part = place_blocks(inverse_blocks(sparse, cosines, SPAN), ROWS, KV_WIDTH, SPAN)
        return (totals + sparse, blended - own_part)
    start_sum = jnp.zeros((n_spans, SPAN * SPAN), jnp.float32)
    totals, new_momentum = lax.scan(replica_step, start_sum, (momentum, gradient, indices))
    update = place_blocks(normalized(inverse_blocks(totals, cosines, SPAN)), ROWS, KV_WIDTH, SPAN)
    return (new_momentum, update)
```

```python
import functools
import math

import jax
import jax.numpy as jnp
import numpy as np
from jax import lax
from jax.experimental import pallas as pl
from jax.experimental.pallas import tpu as pltpu
from jax.sharding import PartitionSpec as P

SPAN = 64
LANES = 128
MESH = pl.DeviceIdType.MESH
F32 = jnp.float32
BF16 = jnp.bfloat16


def cosine_blocks(copies):
    orders = np.arange(SPAN, dtype=np.float64)
    wave, cell = orders[:, None], orders[None, :]
    factor = np.where(wave == 0, math.sqrt(1 / SPAN), math.sqrt(2 / SPAN))
    table = factor * np.cos(math.pi * (2 * cell + 1) * wave / (2 * SPAN))
    full = np.kron(np.eye(copies), table)
    high = full.astype(BF16)
    low = (full - high.astype(np.float64)).astype(BF16)
    return np.stack([high.T, low.T, high, low])


def halves(x):
    high = x.astype(BF16)
    return high, (x - high.astype(F32)).astype(BF16)


def mm(a, b):
    return lax.dot_general(a, b, (((1,), (0,)), ((), ())), preferred_element_type=F32)


def mm_nt(a, b):
    return lax.dot_general(a, b, (((1,), (1,)), ((), ())), preferred_element_type=F32)


def both_sides(blocks, left, right):
    outs = []
    for x in blocks:
        high, low = halves(x)
        y = mm(high, right[0]) + (mm(low, right[0]) + mm(high, right[1]))
        high, low = halves(y)
        outs.append(mm(left[0], high) + (mm(left[0], low) + mm(left[1], high)))
    return outs


def kernel(
    nodes, chips, topk, mom_hbm, grad_hbm, idx_hbm, cos_hbm, new_out, acc, cos,
    mom, grad, idx, box, recv, in_sem, send_sem, recv_sem,
):
    node, chip = lax.axis_index("node"), lax.axis_index("chip")
    count = nodes * chips
    rows, cols = mom.shape
    per = LANES // topk
    wide = per * SPAN
    groups = idx.shape[0] // per
    strips = cols // wide
    batch = math.gcd(nodes, per)
    turn = node % batch

    loads = [
        pltpu.make_async_copy(src, dst, in_sem.at[i])
        for i, (src, dst) in enumerate(
            (
                (idx_hbm.at[0], idx),
                (cos_hbm.at[pl.ds(0, 2)], cos.at[pl.ds(0, 2)]),
                (mom_hbm.at[0], mom),
                (grad_hbm.at[0], grad),
                (cos_hbm.at[pl.ds(2, 2)], cos.at[pl.ds(2, 2)]),
            )
        )
    ]
    for load in loads:
        load.start()

    barrier = pltpu.get_barrier_semaphore()

    half = nodes // 2 if nodes % (2 * batch) == 0 else nodes
    high_side = 2 * chip >= chips

    def plane(t):
        up = t + (chip <= t).astype(jnp.int32)
        down = chips - 1 - t
        return jnp.where(high_side, up, down - (down <= chip).astype(jnp.int32))

    def peers(visit):
        def one(to_chip, i):
            spot = nodes - 1 - node + i
            spot = jnp.where(spot >= nodes, spot - nodes, spot)

            @pl.when((to_chip != chip) | (spot != node))
            def _():
                visit({"node": spot, "chip": to_chip})

        for to_chip in range(chips):
            go = functools.partial(one, to_chip)
            if nodes <= 8:
                for i in range(nodes):
                    go(i)
            else:
                pl.loop(0, nodes)(go)

    peers(lambda to: pl.semaphore_signal(barrier, inc=1, device_id=to, device_id_type=MESH))

    loads[0].wait()
    slots = idx[...]
    spans = slots.shape[0]
    lane = lax.broadcasted_iota(jnp.int32, (spans, LANES), 1)
    place = lax.broadcasted_iota(jnp.int32, (spans, LANES), 0) % per
    spread = jnp.concatenate([slots] * per, axis=1)
    spread = jnp.where(lane // topk == (place + turn) % per, spread + place * (SPAN * SPAN), 0)
    lists = [
        jnp.sum(spread[g * per:(g + 1) * per], axis=0, keepdims=True) for g in range(groups)
    ]
    wave = [(x // SPAN) % SPAN for x in lists]
    wide_pos = [(x // (SPAN * SPAN)) * SPAN + x % SPAN for x in lists]
    tall_iota = lax.broadcasted_iota(jnp.int32, (SPAN, LANES), 0)
    wide_iota = lax.broadcasted_iota(jnp.int32, (wide, LANES), 0)
    wave_hot = [(tall_iota == w).astype(F32).astype(BF16) for w in wave]
    wide_hot = [(wide_iota == w).astype(F32).astype(BF16) for w in wide_pos]

    loads[1].wait()
    tall_cos = [
        mm(cos[0, :SPAN, :SPAN], hot) + mm(cos[1, :SPAN, :SPAN], hot) for hot in wave_hot
    ]
    edge = cos.shape[-1]

    def columns(table, hot):
        pieces = [mm(table, hot[p:p + edge]).astype(BF16) for p in range(0, wide, edge)]
        return jnp.concatenate(pieces, axis=0)

    wide_high = [columns(cos[0], hot) for hot in wide_hot]
    wide_low = [columns(cos[1], hot) for hot in wide_hot]

    loads[2].wait()
    loads[3].wait()
    blended = 0.9 * mom[...] + grad[...].astype(F32)

    def part(g):
        a, s = g // strips, g % strips
        return a, s

    def region(g):
        a, s = part(g)
        return slice(a * SPAN, (a + 1) * SPAN), slice(s * wide, (s + 1) * wide)

    picked = []
    for g in range(groups):
        high, low = halves(blended[region(g)])
        sums = mm(high, wide_high[g]) + (mm(low, wide_high[g]) + mm(high, wide_low[g]))
        picked.append(jnp.sum(sums * tall_cos[g], axis=0, keepdims=True))
    codes = [
        (1 + w.astype(F32) / SPAN) * jnp.exp2((x % SPAN).astype(F32) - SPAN // 2)
        for w, x in zip(wave, lists)
    ]
    payload = jnp.concatenate(picked + codes, axis=0).astype(BF16)
    me = chip * nodes + node
    box[...] = payload
    recv[me] = payload

    pl.semaphore_wait(barrier, count - 1)
    peers(
        lambda to: pltpu.make_async_remote_copy(
            src_ref=box,
            dst_ref=recv.at[me],
            send_sem=send_sem,
            recv_sem=recv_sem.at[chip, node // half],
            device_id=to,
            device_id_type=MESH,
        ).start()
    )

    for g in range(groups):
        sent_value = picked[g].astype(BF16).astype(F32)
        high, low = halves(tall_cos[g] * sent_value)
        own_part = mm_nt(high, wide_high[g]) + (
            mm_nt(low, wide_high[g]) + mm_nt(high, wide_low[g])
        )
        new_out[region(g)] = blended[region(g)] - own_part

    acc[...] = jnp.zeros_like(acc)
    tall_ids = tall_iota.astype(F32).astype(BF16)
    one, zero = jnp.ones((), BF16), jnp.zeros((), BF16)
    blank = jnp.zeros((SPAN, LANES), BF16)
    part_row = lax.broadcasted_iota(jnp.int32, (2 * groups, LANES), 0)
    part_lane = lax.broadcasted_iota(jnp.int32, (2 * groups, LANES), 1) // topk
    empty = (part_row >= groups).astype(F32)

    def decode(start):
        rows = [recv[start + q].astype(F32) for q in range(batch)]
        merged = []
        for p in range(per):
            m = empty
            for q in range(batch):
                m = jnp.where(part_lane == (p + q) % per, rows[q], m)
            power = jnp.floor(jnp.log2(m) + 1 / SPAN / 4)
            col = power + SPAN // 2
            row = jnp.floor((m * jnp.exp2(-power) - 1) * SPAN + 0.5)
            merged.append((m.astype(BF16), row.astype(BF16), col.astype(BF16)))
        for g in range(groups):
            a, s = part(g)
            for p in range(0, per, 2):
                left, right = [], []
                for val, row, col in merged[p:p + 2]:
                    left.append(jnp.where(tall_ids == row[groups + g:groups + g + 1], val[g:g + 1], zero))
                    right.append(jnp.where(tall_ids == col[groups + g:groups + g + 1], one, zero))
                right = jnp.concatenate(
                    [jnp.concatenate([right[0], blank], axis=1), jnp.concatenate([blank, right[1]], axis=1)], axis=0
                )
                acc[pl.ds(a * SPAN, SPAN), pl.ds(s * wide + p * SPAN, 2 * SPAN)] += mm_nt(
                    jnp.concatenate(left, axis=1), right
                )

    for t in reversed(range(chips)):
        source = chip if t == chips - 1 else plane(t)
        for h in range(nodes // half):
            part_no = lax.rem(node // half + h, nodes // half)
            first = source * nodes + part_no * half
            own = t == chips - 1 and h == 0
            if not (own and half == 1):
                landed = recv.at[pl.ds(first, half - 1 if own else half)]
                pltpu.make_async_copy(landed, landed, recv_sem.at[source, part_no]).wait()
            if half == batch:
                decode(first)
            else:
                pl.loop(0, half // batch)(lambda i: decode(first + i * batch))

    loads[4].wait()
    sent = recv.at[pl.ds(0, count - 1)]
    pltpu.make_async_copy(sent, sent, send_sem).wait()


def finish(new_in, acc, cos, new_hbm, upd_hbm, upd, sem):
    store_new = pltpu.make_async_copy(new_in, new_hbm.at[0], sem.at[0])
    store_new.start()
    rows, cols = acc.shape
    wide = cos.shape[-1]
    strips = cols // wide
    totals = [acc[:, s * wide:(s + 1) * wide] for s in range(strips)]
    same = (
        lax.broadcasted_iota(jnp.int32, (wide, wide), 0) // SPAN
        == lax.broadcasted_iota(jnp.int32, (wide, wide), 1) // SPAN
    ).astype(F32).astype(BF16)
    left = (cos[0, :rows, :rows], cos[1, :rows, :rows])
    stores = [store_new]
    for s in range(strips):
        scales = []
        for a in range(rows // SPAN):
            power = totals[s][a * SPAN:(a + 1) * SPAN]
            power = jnp.sum((power * power).reshape(SPAN // 8, 8, wide), axis=0)
            high, low = halves(power)
            energy = jnp.sum(mm(high, same) + mm(low, same), axis=0, keepdims=True)
            scales.append(1.0 / jnp.sqrt(energy * (1.0 / (SPAN * SPAN)) + 1.0))
        field = both_sides([totals[s]], left, (cos[2], cos[3]))[0]
        cut = pl.ds(s * wide, wide)
        for a, scale in enumerate(scales):
            band = slice(a * SPAN, (a + 1) * SPAN)
            upd[band, s * wide:(s + 1) * wide] = field[band] * scale
        store = pltpu.make_async_copy(upd.at[:, cut], upd_hbm.at[:, cut], sem.at[1 + s])
        store.start()
        stores.append(store)
    for store in stores:
        store.wait()


def solution(mesh):
    nodes, chips = mesh.shape["node"], mesh.shape["chip"]

    def step(momentum, gradient, indices):
        _, rows, cols = momentum.shape
        spans, topk = indices.shape[1:]
        per = LANES // topk
        wide = per * SPAN
        used = 2 * (spans // per)
        cosines = jnp.asarray(cosine_blocks(2))
        hbm = pl.BlockSpec(memory_space=pltpu.HBM)
        vmem = pl.BlockSpec(memory_space=pltpu.VMEM)
        new_momentum, totals, tables = pl.pallas_call(
            functools.partial(kernel, nodes, chips, topk),
            out_shape=(
                pltpu.VMEM((rows, cols), F32),
                pltpu.VMEM((rows, cols), F32),
                pltpu.VMEM((4, 2 * SPAN, 2 * SPAN), BF16),
            ),
            in_specs=[hbm] * 4,
            out_specs=(vmem, vmem, vmem),
            scratch_shapes=[
                pltpu.VMEM((rows, cols), F32),
                pltpu.VMEM((rows, cols), BF16),
                pltpu.VMEM((spans, topk), jnp.int32),
                pltpu.VMEM((used, LANES), BF16),
                pltpu.VMEM((nodes * chips, used, LANES), BF16),
                pltpu.SemaphoreType.DMA((5,)),
                pltpu.SemaphoreType.DMA,
                pltpu.SemaphoreType.DMA((chips, 2)),
            ],
            compiler_params=pltpu.CompilerParams(
                collective_id=0, has_side_effects=True, vmem_limit_bytes=24 * 2**20
            ),
        )(*(pltpu.with_memory_space_constraint(x, pltpu.HBM) for x in (momentum, gradient, indices, cosines)))
        return tuple(pl.pallas_call(
            finish,
            out_shape=(
                jax.ShapeDtypeStruct((1, rows, cols), F32),
                jax.ShapeDtypeStruct((rows, cols), F32),
            ),
            in_specs=[vmem, vmem, vmem],
            out_specs=(hbm, hbm),
            scratch_shapes=[
                pltpu.VMEM((rows, cols), F32),
                pltpu.SemaphoreType.DMA((1 + cols // (2 * SPAN),)),
            ],
            compiler_params=pltpu.CompilerParams(vmem_limit_bytes=24 * 2**20),
        )(new_momentum, totals, tables))

    return jax.shard_map(
        step,
        mesh=mesh,
        in_specs=(P(("node", "chip"), None, None),) * 3,
        out_specs=(P(("node", "chip"), None, None), P()),
        check_vma=False,
    )
```

```python
import functools
import math

import jax
import jax.numpy as jnp
import numpy as np
from jax import lax
from jax.experimental import pallas as pl
from jax.experimental.pallas import tpu as pltpu
from jax.sharding import PartitionSpec as P

SPAN = 64
LANES = 128
MESH = pl.DeviceIdType.MESH
F32 = jnp.float32
BF16 = jnp.bfloat16


def cosine_tables():
    orders = np.arange(SPAN, dtype=np.float64)
    wave, cell = orders[:, None], orders[None, :]
    factor = np.where(wave == 0, math.sqrt(1 / SPAN), math.sqrt(2 / SPAN))
    table = factor * np.cos(math.pi * (2 * cell + 1) * wave / (2 * SPAN))
    high = table.astype(BF16)
    low = (table - high.astype(np.float64)).astype(BF16)
    pair = np.eye(LANES // SPAN, dtype=BF16)
    right = np.concatenate([np.kron(pair, high), np.kron(pair, low)], axis=1)
    left = np.concatenate([high.T, high.T, low.T, np.zeros_like(low)], axis=1)
    pick = np.pad(np.concatenate([high.T, low.T], axis=0), ((0, 0), (0, LANES - SPAN)))
    return pick, np.concatenate([right, right], axis=0), left


def halves(x):
    high = x.astype(BF16)
    return high, (x - high.astype(F32)).astype(BF16)


def mm(a, b):
    return lax.dot_general(a, b, (((1,), (0,)), ((), ())), preferred_element_type=F32)


def mm_nt(a, b):
    return lax.dot_general(a, b, (((1,), (1,)), ((), ())), preferred_element_type=F32)


def kernel(
    nodes, chips, topk, mom_hbm, grad_hbm, idx_hbm, pick_hbm, right_hbm, left_hbm, new_out, acc,
    right_cos, left_cos, pick, mom, grad, idx, box, recv, in_sem, send_sem, recv_sem,
):
    node, chip = lax.axis_index("node"), lax.axis_index("chip")
    count = nodes * chips
    rows, cols = mom.shape
    per = LANES // topk
    wide = per * SPAN
    groups = idx.shape[0] // per
    strips = cols // wide
    batch = math.gcd(nodes, per)
    turn = node % batch

    bands = rows // SPAN
    loads = [(idx_hbm.at[0], idx), (pick_hbm, pick)]
    for a in range(bands):
        band = pl.ds(a * SPAN, SPAN)
        loads += [(mom_hbm.at[0, band], mom.at[band]), (grad_hbm.at[0, band], grad.at[band])]
    loads += [(right_hbm, right_cos), (left_hbm, left_cos)]
    loads = [pltpu.make_async_copy(*x, in_sem.at[i]) for i, x in enumerate(loads)]
    for load in loads[:-2]:
        load.start()

    barrier = pltpu.get_barrier_semaphore()

    unit = 2 * batch if nodes % (2 * batch) == 0 else batch
    high_side = 2 * chip >= chips

    def plane(t):
        up = t + (chip <= t).astype(jnp.int32)
        down = chips - 1 - t
        return jnp.where(high_side, up, down - (down <= chip).astype(jnp.int32))

    def peers(visit):
        def one(to_chip, i):
            spot = nodes - 1 - node + i
            spot = jnp.where(spot >= nodes, spot - nodes, spot)

            @pl.when((to_chip != chip) | (spot != node))
            def _():
                visit({"node": spot, "chip": to_chip})

        for to_chip in range(chips):
            go = functools.partial(one, to_chip)
            if nodes <= 8:
                for i in range(nodes):
                    go(i)
            else:
                pl.loop(0, nodes)(go)

    def greet(to_chip, spot):
        pl.semaphore_signal(
            barrier, inc=1, device_id={"node": spot, "chip": to_chip}, device_id_type=MESH
        )

    def greet_own(i):
        spot = node + i
        greet(chip, jnp.where(spot >= nodes, spot - nodes, spot))

    for to_chip in map(plane, range(chips - 1)):
        if nodes <= 8:
            for spot in range(nodes):
                greet(to_chip, spot)
        else:
            pl.loop(0, nodes)(functools.partial(greet, to_chip))
    if nodes <= 8:
        for i in range(1, nodes):
            greet_own(i)
    else:
        pl.loop(1, nodes)(greet_own)

    loads[0].wait()
    slots = idx[...]
    spans = slots.shape[0]
    lane = lax.broadcasted_iota(jnp.int32, (spans, LANES), 1)
    place = lax.broadcasted_iota(jnp.int32, (spans, LANES), 0) % per
    spread = jnp.concatenate([slots] * per, axis=1)
    spread = jnp.where(lane // topk == (place + turn) % per, spread + place * (SPAN * SPAN), 0)
    lists = [
        jnp.sum(spread[g * per:(g + 1) * per], axis=0, keepdims=True) for g in range(groups)
    ]
    one, zero = jnp.ones((), BF16), jnp.zeros((), BF16)
    tall_ids = lax.broadcasted_iota(jnp.int32, (SPAN, LANES), 0).astype(F32).astype(BF16)
    wave = [((x // SPAN) % SPAN).astype(F32) for x in lists]
    cell = [(x % SPAN).astype(F32) for x in lists]
    hot = [jnp.where(tall_ids == x.astype(BF16), one, zero) for x in cell + wave]

    loads[1].wait()
    found = mm(pick[:, :SPAN], jnp.concatenate(hot, axis=1))
    found = [found[:, g * LANES:(g + 1) * LANES] for g in range(2 * groups)]
    tall_cos = [x[:SPAN] + x[SPAN:] for x in found[groups:]]
    seat = (lax.broadcasted_iota(jnp.int32, (SPAN, LANES), 1) // topk + per - turn) % per

    def columns(x):
        x = x.astype(BF16)
        return jnp.concatenate([jnp.where(seat == p, x, zero) for p in range(per)], axis=0)

    wide_high = [columns(x[:SPAN]) for x in found[:groups]]
    wide_low = [columns(x[SPAN:]) for x in found[:groups]]

    blended, picked = [], []
    for load in loads[2:-2]:
        load.wait()
    for a in range(bands):
        band = slice(a * SPAN, (a + 1) * SPAN)
        for b in range(strips):
            g = a * strips + b
            strip = slice(b * wide, (b + 1) * wide)
            blended.append(0.9 * mom[band, strip] + grad[band, strip].astype(F32))
            sums = mm(
                jnp.concatenate(halves(blended[g]), axis=0),
                jnp.concatenate([wide_high[g], wide_low[g]], axis=1),
            )
            sums = sums[:SPAN, :LANES] + (sums[SPAN:, :LANES] + sums[:SPAN, LANES:])
            picked.append(jnp.sum(sums * tall_cos[g], axis=0, keepdims=True))
    codes = [(1 + w / SPAN) * jnp.exp2(c - SPAN // 2) for w, c in zip(wave, cell)]
    payload = jnp.concatenate(picked + codes, axis=0).astype(BF16)
    me = chip * nodes + node
    box[...] = payload
    recv[me] = payload

    pl.semaphore_wait(barrier, count - 1)
    peers(
        lambda to: pltpu.make_async_remote_copy(
            src_ref=box,
            dst_ref=recv.at[me],
            send_sem=send_sem,
            recv_sem=recv_sem.at[chip],
            device_id=to,
            device_id_type=MESH,
        ).start()
    )

    for load in loads[-2:]:
        load.start()

    for g in range(groups):
        sent_value = picked[g].astype(BF16).astype(F32)
        high, low = halves(tall_cos[g] * sent_value)
        own_part = mm_nt(high, wide_high[g]) + (
            mm_nt(low, wide_high[g]) + mm_nt(high, wide_low[g])
        )
        a, b = g // strips, g % strips
        new_out[a * SPAN:(a + 1) * SPAN, b * wide:(b + 1) * wide] = blended[g] - own_part

    part_row = lax.broadcasted_iota(jnp.int32, (2 * groups, LANES), 0)
    part_lane = lax.broadcasted_iota(jnp.int32, (2 * groups, LANES), 1) // topk
    empty = (part_row >= groups).astype(F32)

    def entries(start):
        rows = [recv[start + q].astype(F32) for q in range(batch)]
        hots = []
        for p in range(per):
            m = empty
            for q in range(batch):
                m = jnp.where(part_lane == (p + q) % per, rows[q], m)
            power = jnp.floor(jnp.log2(m) + 1 / SPAN / 4)
            col = (power + SPAN // 2).astype(BF16)
            row = jnp.floor((m * jnp.exp2(-power) - 1) * SPAN + 0.5).astype(BF16)
            hots.append((m.astype(BF16), row, col))

        def hot(g, p):
            val, row, col = hots[p]
            at = groups + g
            return (
                jnp.where(tall_ids == row[at:at + 1], val[g:g + 1], zero),
                jnp.where(tall_ids == col[at:at + 1], one, zero),
            )

        return hot

    def decode(start, totals):
        hots = [entries(start + i) for i in range(0, unit, batch)]
        sums = []
        for c in range(spans):
            left, right = zip(*(hot(c // per, c % per) for hot in hots))
            sums.append(
                totals[c] + mm_nt(jnp.concatenate(left, axis=1), jnp.concatenate(right, axis=1))
            )
        return sums

    for load in loads[-2:]:
        load.wait()
    sent = recv.at[pl.ds(0, count - 1)]
    totals = [jnp.zeros((SPAN, SPAN), F32)] * spans
    for t in reversed(range(chips)):
        source = chip if t == chips - 1 else plane(t)
        first = source * nodes
        if t == 0:
            pltpu.make_async_copy(sent, sent, send_sem).wait()
        landed = recv.at[pl.ds(first, nodes - 1 if t == chips - 1 else nodes)]
        pltpu.make_async_copy(landed, landed, recv_sem.at[source]).wait()
        if unit == nodes:
            totals = decode(first, totals)
        else:
            totals = lax.fori_loop(
                0, nodes // unit, lambda i, old: decode(first + i * unit, old), totals
            )
    for c in range(0, spans, 2):
        acc[c // 2 * SPAN:(c // 2 + 1) * SPAN] = jnp.concatenate(totals[c:c + 2], axis=1)


def finish(new_in, acc, right_cos, left_cos, new_hbm, upd_hbm, upd, sem):
    store_new = pltpu.make_async_copy(new_in, new_hbm.at[0], sem.at[0])
    store_new.start()
    rows, cols = upd.shape
    strips = cols // (2 * LANES)
    turned = mm(jnp.concatenate(halves(acc[...]), axis=1), right_cos[...])
    turned = turned[:, :LANES] + turned[:, LANES:]
    pairs = acc.shape[0] // SPAN
    same = (
        lax.broadcasted_iota(jnp.int32, (LANES, LANES), 0) // SPAN
        == lax.broadcasted_iota(jnp.int32, (LANES, LANES), 1) // SPAN
    ).astype(F32).astype(BF16)
    blocks = [acc[c * SPAN:(c + 1) * SPAN] for c in range(pairs)]
    power = jnp.concatenate([jnp.sum(x * x, axis=0, keepdims=True) for x in blocks], axis=0)
    energy = mm(jnp.concatenate(halves(power), axis=0), same)
    energy = energy[:pairs] + energy[pairs:]
    scale = 1.0 / jnp.sqrt(energy * (1.0 / (SPAN * SPAN)) + 1.0)
    stores = [store_new]
    for c in range(0, pairs, 2):
        pieces = [turned[d * SPAN:(d + 1) * SPAN] for d in (c, c + 1)]
        high, low = halves(jnp.concatenate(pieces, axis=1))
        field = mm(left_cos[:, :3 * SPAN], jnp.concatenate([high, low, high], axis=0))
        level = jnp.concatenate([scale[c:c + 1], scale[c + 1:c + 2]], axis=1)
        a, s = c // 2 // strips, c // 2 % strips
        cut = pl.ds(a * SPAN, SPAN), pl.ds(s * 2 * LANES, 2 * LANES)
        upd[cut] = field * level
        store = pltpu.make_async_copy(upd.at[cut], upd_hbm.at[cut], sem.at[1 + c // 2])
        store.start()
        stores.append(store)
    for store in stores:
        store.wait()


def solution(mesh):
    nodes, chips = mesh.shape["node"], mesh.shape["chip"]

    def step(momentum, gradient, indices):
        _, rows, cols = momentum.shape
        spans, topk = indices.shape[1:]
        per = LANES // topk
        wide = per * SPAN
        used = 2 * (spans // per)
        tables = [jnp.asarray(x) for x in cosine_tables()]
        hbm = pl.BlockSpec(memory_space=pltpu.HBM)
        vmem = pl.BlockSpec(memory_space=pltpu.VMEM)
        operands = [momentum, gradient, indices, *tables]
        results = pl.pallas_call(
            functools.partial(kernel, nodes, chips, topk),
            out_shape=(
                pltpu.VMEM((rows, cols), F32),
                pltpu.VMEM((rows * cols // LANES, LANES), F32),
                *(pltpu.VMEM(x.shape, BF16) for x in tables[1:]),
            ),
            in_specs=[hbm] * 6,
            out_specs=(vmem,) * 4,
            scratch_shapes=[
                pltpu.VMEM(tables[0].shape, BF16),
                pltpu.VMEM((rows, cols), F32),
                pltpu.VMEM((rows, cols), BF16),
                pltpu.VMEM((spans, topk), jnp.int32),
                pltpu.VMEM((used, LANES), BF16),
                pltpu.VMEM((nodes * chips, used, LANES), BF16),
                pltpu.SemaphoreType.DMA((4 + 2 * (rows // SPAN),)),
                pltpu.SemaphoreType.DMA,
                pltpu.SemaphoreType.DMA((chips,)),
            ],
            compiler_params=pltpu.CompilerParams(
                collective_id=0, has_side_effects=True, vmem_limit_bytes=24 * 2**20
            ),
        )(*(pltpu.with_memory_space_constraint(x, pltpu.HBM) for x in operands))
        return tuple(pl.pallas_call(
            finish,
            out_shape=(
                jax.ShapeDtypeStruct((1, rows, cols), F32),
                jax.ShapeDtypeStruct((rows, cols), F32),
            ),
            in_specs=[vmem] * 4,
            out_specs=(hbm, hbm),
            scratch_shapes=[
                pltpu.VMEM((rows, cols), F32),
                pltpu.SemaphoreType.DMA((1 + spans // 4,)),
            ],
            compiler_params=pltpu.CompilerParams(vmem_limit_bytes=24 * 2**20),
        )(*results))

    return jax.shard_map(
        step,
        mesh=mesh,
        in_specs=(P(("node", "chip"), None, None),) * 3,
        out_specs=(P(("node", "chip"), None, None), P()),
        check_vma=False,
    )
```

```python
import functools
import math

import jax
import jax.numpy as jnp
import numpy as np
from jax import lax
from jax.experimental import pallas as pl
from jax.experimental.pallas import tpu as pltpu
from jax.sharding import PartitionSpec as P

SPAN = 64
LANES = 128
MESH = pl.DeviceIdType.MESH
F32 = jnp.float32
BF16 = jnp.bfloat16


def cosine_tables():
    orders = np.arange(SPAN, dtype=np.float64)
    wave, cell = orders[:, None], orders[None, :]
    factor = np.where(wave == 0, math.sqrt(1 / SPAN), math.sqrt(2 / SPAN))
    table = factor * np.cos(math.pi * (2 * cell + 1) * wave / (2 * SPAN))
    high = table.astype(BF16)
    low = (table - high.astype(np.float64)).astype(BF16)
    pair = np.eye(LANES // SPAN, dtype=BF16)
    right = np.concatenate([np.kron(pair, high), np.kron(pair, low)], axis=1)
    left = np.concatenate([high.T, high.T, low.T, np.zeros_like(low)], axis=1)
    pick = np.pad(np.concatenate([high.T, low.T], axis=0), ((0, 0), (0, LANES - SPAN)))
    return pick, np.concatenate([right, right], axis=0), left


def halves(x):
    high = x.astype(BF16)
    return high, (x - high.astype(F32)).astype(BF16)


def mm(a, b):
    return lax.dot_general(a, b, (((1,), (0,)), ((), ())), preferred_element_type=F32)


def mm_nt(a, b):
    return lax.dot_general(a, b, (((1,), (1,)), ((), ())), preferred_element_type=F32)


def kernel(
    nodes, chips, topk, mom_hbm, grad_hbm, idx_hbm, pick_hbm, right_hbm, left_hbm, new_out, turned,
    scale, left_cos, right_cos, pick, mom, grad, idx, box, recv, in_sem, send_sem, recv_sem,
):
    node, chip = lax.axis_index("node"), lax.axis_index("chip")
    count = nodes * chips
    rows, cols = mom.shape
    per = LANES // topk
    wide = per * SPAN
    groups = idx.shape[0] // per
    strips = cols // wide
    batch = math.gcd(nodes, per)
    turn = node % batch

    bands = rows // SPAN
    loads = [
        (idx_hbm.at[0], idx),
        (pick_hbm, pick),
        (mom_hbm.at[0], mom),
        (grad_hbm.at[0], grad),
        (right_hbm, right_cos),
        (left_hbm, left_cos),
    ]
    loads = [pltpu.make_async_copy(*x, in_sem.at[i]) for i, x in enumerate(loads)]
    for load in loads[:-2]:
        load.start()

    barrier = pltpu.get_barrier_semaphore()

    unit = 2 * batch if nodes % (2 * batch) == 0 else batch
    high_side = 2 * chip >= chips

    def plane(t):
        up = t + (chip <= t).astype(jnp.int32)
        down = chips - 1 - t
        return jnp.where(high_side, up, down - (down <= chip).astype(jnp.int32))

    def peers(visit):
        def one(to_chip, i):
            @pl.when((to_chip != chip) | (i != node))
            def _():
                visit({"node": i, "chip": to_chip})

        for to_chip in range(chips):
            go = functools.partial(one, to_chip)
            if nodes <= 8:
                for i in range(nodes):
                    go(i)
            else:
                pl.loop(0, nodes)(go)

    def greet(to_chip, spot):
        pl.semaphore_signal(
            barrier, inc=1, device_id={"node": spot, "chip": to_chip}, device_id_type=MESH
        )

    def greet_own(i):
        spot = node + i
        greet(chip, jnp.where(spot >= nodes, spot - nodes, spot))

    for to_chip in map(plane, range(chips - 1)):
        if nodes <= 8:
            for spot in range(nodes):
                greet(to_chip, spot)
        else:
            pl.loop(0, nodes)(functools.partial(greet, to_chip))
    if nodes <= 8:
        for i in range(1, nodes):
            greet_own(i)
    else:
        pl.loop(1, nodes)(greet_own)

    loads[0].wait()
    slots = idx[...]
    spans = slots.shape[0]
    lane = lax.broadcasted_iota(jnp.int32, (spans, LANES), 1)
    place = lax.broadcasted_iota(jnp.int32, (spans, LANES), 0) % per
    spread = jnp.concatenate([slots] * per, axis=1)
    spread = jnp.where(lane // topk == (place + turn) % per, spread + place * (SPAN * SPAN), 0)
    lists = [
        jnp.sum(spread[g * per:(g + 1) * per], axis=0, keepdims=True) for g in range(groups)
    ]
    one, zero = jnp.ones((), BF16), jnp.zeros((), BF16)
    tall_ids = lax.broadcasted_iota(jnp.int32, (SPAN, LANES), 0).astype(F32).astype(BF16)
    wave = [((x // SPAN) % SPAN).astype(F32) for x in lists]
    cell = [(x % SPAN).astype(F32) for x in lists]
    hot = [jnp.where(tall_ids == x.astype(BF16), one, zero) for x in cell + wave]

    loads[1].wait()
    found = mm(pick[:, :SPAN], jnp.concatenate(hot, axis=1))
    found = [found[:, g * LANES:(g + 1) * LANES] for g in range(2 * groups)]
    tall_cos = [x[:SPAN] + x[SPAN:] for x in found[groups:]]
    seat = (lax.broadcasted_iota(jnp.int32, (SPAN, LANES), 1) // topk + per - turn) % per

    def columns(x):
        x = x.astype(BF16)
        return jnp.concatenate([jnp.where(seat == p, x, zero) for p in range(per)], axis=0)

    wide_high = [columns(x[:SPAN]) for x in found[:groups]]
    wide_low = [columns(x[SPAN:]) for x in found[:groups]]

    blended, picked = [], []
    for load in loads[2:-2]:
        load.wait()
    for a in range(bands):
        band = slice(a * SPAN, (a + 1) * SPAN)
        for b in range(strips):
            g = a * strips + b
            strip = slice(b * wide, (b + 1) * wide)
            blended.append(0.9 * mom[band, strip] + grad[band, strip].astype(F32))
            sums = mm(
                jnp.concatenate(halves(blended[g]), axis=0),
                jnp.concatenate([wide_high[g], wide_low[g]], axis=1),
            )
            sums = sums[:SPAN, :LANES] + (sums[SPAN:, :LANES] + sums[:SPAN, LANES:])
            picked.append(jnp.sum(sums * tall_cos[g], axis=0, keepdims=True))
    codes = [(1 + w / SPAN) * jnp.exp2(c - SPAN // 2) for w, c in zip(wave, cell)]
    payload = jnp.concatenate(picked + codes, axis=0).astype(BF16)
    me = chip * nodes + node
    box[...] = payload
    recv[me] = payload

    pl.semaphore_wait(barrier, count - 1)
    peers(
        lambda to: pltpu.make_async_remote_copy(
            src_ref=box,
            dst_ref=recv.at[me],
            send_sem=send_sem,
            recv_sem=recv_sem.at[chip],
            device_id=to,
            device_id_type=MESH,
        ).start()
    )

    for load in loads[-2:]:
        load.start()

    for g in range(groups):
        sent_value = picked[g].astype(BF16).astype(F32)
        high, low = halves(tall_cos[g] * sent_value)
        own_part = mm_nt(high, wide_high[g]) + (
            mm_nt(low, wide_high[g]) + mm_nt(high, wide_low[g])
        )
        a, b = g // strips, g % strips
        new_out[a * SPAN:(a + 1) * SPAN, b * wide:(b + 1) * wide] = blended[g] - own_part

    part_row = lax.broadcasted_iota(jnp.int32, (2 * groups, LANES), 0)
    part_lane = lax.broadcasted_iota(jnp.int32, (2 * groups, LANES), 1) // topk
    empty = (part_row >= groups).astype(F32)

    def entries(start):
        rows = [recv[start + q].astype(F32) for q in range(batch)]
        hots = []
        for p in range(per):
            m = empty
            for q in range(batch):
                m = jnp.where(part_lane == (p + q) % per, rows[q], m)
            power = jnp.floor(jnp.log2(m) + 1 / SPAN / 4)
            col = (power + SPAN // 2).astype(BF16)
            row = jnp.floor((m * jnp.exp2(-power) - 1) * SPAN + 0.5).astype(BF16)
            hots.append((m.astype(BF16), row, col))

        def hot(g, p):
            val, row, col = hots[p]
            at = groups + g
            return (
                jnp.where(tall_ids == row[at:at + 1], val[g:g + 1], zero),
                jnp.where(tall_ids == col[at:at + 1], one, zero),
            )

        return hot

    def decode(start, totals):
        hots = [entries(start + i) for i in range(0, unit, batch)]
        sums = []
        for c in range(spans):
            left, right = zip(*(hot(c // per, c % per) for hot in hots))
            sums.append(
                totals[c] + mm_nt(jnp.concatenate(left, axis=1), jnp.concatenate(right, axis=1))
            )
        return sums

    for load in loads[-2:]:
        load.wait()
    sent = recv.at[pl.ds(0, count - 1)]
    totals = [jnp.zeros((SPAN, SPAN), F32)] * spans
    for t in reversed(range(chips)):
        source = chip if t == chips - 1 else plane(t)
        first = source * nodes
        if t == 0:
            pltpu.make_async_copy(sent, sent, send_sem).wait()
        landed = recv.at[pl.ds(first, nodes - 1 if t == chips - 1 else nodes)]
        pltpu.make_async_copy(landed, landed, recv_sem.at[source]).wait()
        if unit == nodes:
            totals = decode(first, totals)
        else:
            totals = lax.fori_loop(
                0, nodes // unit, lambda i, old: decode(first + i * unit, old), totals
            )
    pairs = [jnp.concatenate(totals[c:c + 2], axis=1) for c in range(0, spans, 2)]
    chunk = max(1, len(pairs) // 2)
    for c in range(0, len(pairs), chunk):
        both = jnp.concatenate(halves(jnp.concatenate(pairs[c:c + chunk], axis=0)), axis=1)
        both = mm(both, right_cos[...])
        turned[c * SPAN:(c + chunk) * SPAN] = both[:, :LANES] + both[:, LANES:]
    same = (
        lax.broadcasted_iota(jnp.int32, (LANES, LANES), 0) // SPAN
        == lax.broadcasted_iota(jnp.int32, (LANES, LANES), 1) // SPAN
    ).astype(F32).astype(BF16)
    power = jnp.concatenate([jnp.sum(x * x, axis=0, keepdims=True) for x in pairs], axis=0)
    energy = mm(jnp.concatenate(halves(power), axis=0), same)
    energy = energy[:len(pairs)] + energy[len(pairs):]
    scale[...] = 1.0 / jnp.sqrt(energy * (1.0 / (SPAN * SPAN)) + 1.0)


def finish(new_in, turned, scale, left_cos, new_hbm, upd_hbm, upd, sem):
    store_new = pltpu.make_async_copy(new_in, new_hbm.at[0], sem.at[0])
    store_new.start()
    strips = upd.shape[1] // (2 * LANES)
    stores = [store_new]
    for c in range(0, scale.shape[0], 2):
        pieces = [turned[d * SPAN:(d + 1) * SPAN] for d in (c, c + 1)]
        high, low = halves(jnp.concatenate(pieces, axis=1))
        field = mm(left_cos[:, :3 * SPAN], jnp.concatenate([high, low, high], axis=0))
        level = jnp.concatenate([scale[c:c + 1], scale[c + 1:c + 2]], axis=1)
        a, s = c // 2 // strips, c // 2 % strips
        cut = pl.ds(a * SPAN, SPAN), pl.ds(s * 2 * LANES, 2 * LANES)
        upd[cut] = field * level
        store = pltpu.make_async_copy(upd.at[cut], upd_hbm.at[cut], sem.at[1 + c // 2])
        store.start()
        stores.append(store)
    for store in stores:
        store.wait()


def solution(mesh):
    nodes, chips = mesh.shape["node"], mesh.shape["chip"]

    def step(momentum, gradient, indices):
        _, rows, cols = momentum.shape
        spans, topk = indices.shape[1:]
        per = LANES // topk
        wide = per * SPAN
        used = 2 * (spans // per)
        tables = [jnp.asarray(x) for x in cosine_tables()]
        hbm = pl.BlockSpec(memory_space=pltpu.HBM)
        vmem = pl.BlockSpec(memory_space=pltpu.VMEM)
        operands = [momentum, gradient, indices, *tables]
        results = pl.pallas_call(
            functools.partial(kernel, nodes, chips, topk),
            out_shape=(
                pltpu.VMEM((rows, cols), F32),
                pltpu.VMEM((rows * cols // LANES, LANES), F32),
                pltpu.VMEM((spans // 2, LANES), F32),
                pltpu.VMEM(tables[2].shape, BF16),
            ),
            in_specs=[hbm] * 6,
            out_specs=(vmem,) * 4,
            scratch_shapes=[
                pltpu.VMEM(tables[1].shape, BF16),
                pltpu.VMEM(tables[0].shape, BF16),
                pltpu.VMEM((rows, cols), F32),
                pltpu.VMEM((rows, cols), BF16),
                pltpu.VMEM((spans, topk), jnp.int32),
                pltpu.VMEM((used, LANES), BF16),
                pltpu.VMEM((nodes * chips, used, LANES), BF16),
                pltpu.SemaphoreType.DMA((6,)),
                pltpu.SemaphoreType.DMA,
                pltpu.SemaphoreType.DMA((chips,)),
            ],
            compiler_params=pltpu.CompilerParams(
                collective_id=0, has_side_effects=True, vmem_limit_bytes=24 * 2**20
            ),
        )(*(pltpu.with_memory_space_constraint(x, pltpu.HBM) for x in operands))
        return tuple(pl.pallas_call(
            finish,
            out_shape=(
                jax.ShapeDtypeStruct((1, rows, cols), F32),
                jax.ShapeDtypeStruct((rows, cols), F32),
            ),
            in_specs=[vmem] * 4,
            out_specs=(hbm, hbm),
            scratch_shapes=[
                pltpu.VMEM((rows, cols), F32),
                pltpu.SemaphoreType.DMA((1 + spans // 4,)),
            ],
            compiler_params=pltpu.CompilerParams(vmem_limit_bytes=24 * 2**20),
        )(*results))

    return jax.shard_map(
        step,
        mesh=mesh,
        in_specs=(P(("node", "chip"), None, None),) * 3,
        out_specs=(P(("node", "chip"), None, None), P()),
        check_vma=False,
    )
```

```python
import functools
import math

import jax
import jax.numpy as jnp
import numpy as np
from jax import lax
from jax.experimental import pallas as pl
from jax.experimental.pallas import tpu as pltpu
from jax.sharding import PartitionSpec as P

SPAN = 64
LANES = 128
MESH = pl.DeviceIdType.MESH
F32 = jnp.float32
BF16 = jnp.bfloat16


def cosine_tables():
    orders = np.arange(SPAN, dtype=np.float64)
    wave, cell = orders[:, None], orders[None, :]
    factor = np.where(wave == 0, math.sqrt(1 / SPAN), math.sqrt(2 / SPAN))
    table = factor * np.cos(math.pi * (2 * cell + 1) * wave / (2 * SPAN))
    high = table.astype(BF16)
    low = (table - high.astype(np.float64)).astype(BF16)
    pair = np.eye(LANES // SPAN, dtype=BF16)
    right = np.concatenate([np.kron(pair, high), np.kron(pair, low)], axis=1)
    left = np.concatenate([high.T, high.T, low.T, np.zeros_like(low)], axis=1)
    pick = np.pad(table.T, ((0, 0), (0, LANES - SPAN))).astype(F32)
    return pick, np.concatenate([right, right], axis=0), left


def halves(x):
    high = x.astype(BF16)
    return high, (x - high.astype(F32)).astype(BF16)


def mm(a, b):
    return lax.dot_general(a, b, (((1,), (0,)), ((), ())), preferred_element_type=F32)


def mm_nt(a, b):
    return lax.dot_general(a, b, (((1,), (1,)), ((), ())), preferred_element_type=F32)


def kernel(
    nodes, chips, topk, mom_hbm, grad_hbm, idx_hbm, pick_hbm, right_hbm, left_hbm, new_out, turned,
    power, left_cos, right_cos, pick, mom, grad, idx, box, recv, in_sem, send_sem, recv_sem,
):
    node, chip = lax.axis_index("node"), lax.axis_index("chip")
    devices = nodes * chips
    rows, cols = mom.shape
    per = LANES // topk
    wide = per * SPAN
    groups = idx.shape[0] // per
    strips = cols // wide
    batch = math.gcd(nodes, per)
    turn = node % batch

    bands = rows // SPAN
    loads = [
        (idx_hbm.at[0], idx),
        (pick_hbm, pick),
        (mom_hbm.at[0], mom),
        (grad_hbm.at[0], grad),
        (right_hbm, right_cos),
        (left_hbm, left_cos),
    ]
    loads = [pltpu.make_async_copy(*x, in_sem.at[i]) for i, x in enumerate(loads)]
    for load in loads[:2]:
        load.start()
    for src, dst, sem, priority, count in (
        (mom_hbm.at[0], mom, in_sem.at[2], 1, 8),
        (grad_hbm.at[0], grad, in_sem.at[3], 0, 4),
    ):
        for i in range(count):
            cut = pl.ds(i * rows // count, rows // count)
            pltpu.make_async_copy(src.at[cut], dst.at[cut], sem).start(priority=priority)

    barrier = pltpu.get_barrier_semaphore()

    unit = 2 * batch if nodes % (2 * batch) == 0 else batch
    high_side = 2 * chip >= chips

    def plane(t):
        up = t + (chip <= t).astype(jnp.int32)
        down = chips - 1 - t
        return jnp.where(high_side, up, down - (down <= chip).astype(jnp.int32))

    def peers(visit):
        def one(to_chip, i):
            @pl.when((to_chip != chip) | (i != node))
            def _():
                visit({"node": i, "chip": to_chip})

        for to_chip in range(chips):
            go = functools.partial(one, to_chip)
            if nodes <= 8:
                for i in range(nodes):
                    go(i)
            else:
                pl.loop(0, nodes)(go)

    def greet(to_chip, spot):
        pl.semaphore_signal(
            barrier, inc=1, device_id={"node": spot, "chip": to_chip}, device_id_type=MESH
        )

    def greet_own(i):
        spot = node + i
        greet(chip, jnp.where(spot >= nodes, spot - nodes, spot))

    for to_chip in map(plane, range(chips - 1)):
        if nodes <= 8:
            for spot in range(nodes):
                greet(to_chip, spot)
        else:
            pl.loop(0, nodes)(functools.partial(greet, to_chip))
    if nodes <= 8:
        for i in range(1, nodes):
            greet_own(i)
    else:
        pl.loop(1, nodes)(greet_own)

    loads[0].wait()
    slots = idx[...]
    spans = slots.shape[0]
    lane = lax.broadcasted_iota(jnp.int32, (spans, LANES), 1)
    place = lax.broadcasted_iota(jnp.int32, (spans, LANES), 0) % per
    spread = jnp.concatenate([slots] * per, axis=1)
    spread = jnp.where(lane // topk == (place + turn) % per, spread + place * (SPAN * SPAN), 0)
    lists = [
        jnp.sum(spread[g * per:(g + 1) * per], axis=0, keepdims=True) for g in range(groups)
    ]
    one, zero = jnp.ones((), BF16), jnp.zeros((), BF16)
    tall_ids = lax.broadcasted_iota(jnp.int32, (SPAN, LANES), 0).astype(F32).astype(BF16)
    wave = [((x // SPAN) % SPAN).astype(F32) for x in lists]
    cell = [(x % SPAN).astype(F32) for x in lists]
    loads[1].wait()

    def gather(row):
        spots = jnp.broadcast_to(row.astype(jnp.int32), (SPAN, LANES))
        return jnp.take_along_axis(pick[...], spots, axis=1, mode="promise_in_bounds")

    found = [halves(gather(x)) for x in cell]
    tall_cos = [gather(x) for x in wave]
    seat = (lax.broadcasted_iota(jnp.int32, (SPAN, LANES), 1) // topk + per - turn) % per

    def columns(x):
        return jnp.concatenate([jnp.where(seat == p, x, zero) for p in range(per)], axis=0)

    wide_high = [columns(x[0]) for x in found]
    wide_low = [columns(x[1]) for x in found]

    blended, picked = [], []
    for load in loads[2:-2]:
        load.wait()
    for a in range(bands):
        band = slice(a * SPAN, (a + 1) * SPAN)
        for b in range(strips):
            g = a * strips + b
            strip = slice(b * wide, (b + 1) * wide)
            blended.append(0.9 * mom[band, strip] + grad[band, strip].astype(F32))
            sums = mm(
                jnp.concatenate(halves(blended[g]), axis=0),
                jnp.concatenate([wide_high[g], wide_low[g]], axis=1),
            )
            sums = sums[:SPAN, :LANES] + (sums[SPAN:, :LANES] + sums[:SPAN, LANES:])
            picked.append(jnp.sum(sums * tall_cos[g], axis=0, keepdims=True))
    codes = [(1 + w / SPAN) * jnp.exp2(c - SPAN // 2) for w, c in zip(wave, cell)]
    payload = jnp.concatenate(picked + codes, axis=0).astype(BF16)
    me = chip * nodes + node
    box[...] = payload
    recv[me] = payload

    pl.semaphore_wait(barrier, devices - 1)
    peers(
        lambda to: pltpu.make_async_remote_copy(
            src_ref=box,
            dst_ref=recv.at[me],
            send_sem=send_sem,
            recv_sem=recv_sem.at[chip],
            device_id=to,
            device_id_type=MESH,
        ).start()
    )

    for load in loads[-2:]:
        load.start()

    for g in range(groups):
        sent_value = picked[g].astype(BF16).astype(F32)
        high, low = halves(tall_cos[g] * sent_value)
        own_part = mm_nt(high, wide_high[g]) + (
            mm_nt(low, wide_high[g]) + mm_nt(high, wide_low[g])
        )
        a, b = g // strips, g % strips
        new_out[a * SPAN:(a + 1) * SPAN, b * wide:(b + 1) * wide] = blended[g] - own_part

    part_row = lax.broadcasted_iota(jnp.int32, (2 * groups, LANES), 0)
    part_lane = lax.broadcasted_iota(jnp.int32, (2 * groups, LANES), 1) // topk
    empty = (part_row >= groups).astype(F32)

    def entries(start):
        rows = [recv[start + q].astype(F32) for q in range(batch)]
        hots = []
        for p in range(per):
            m = empty
            for q in range(batch):
                m = jnp.where(part_lane == (p + q) % per, rows[q], m)
            power = jnp.floor(jnp.log2(m) + 1 / SPAN / 4)
            col = (power + SPAN // 2).astype(BF16)
            row = jnp.floor((m * jnp.exp2(-power) - 1) * SPAN + 0.5).astype(BF16)
            hots.append((m.astype(BF16), row, col))

        def hot(g, p):
            val, row, col = hots[p]
            at = groups + g
            return (
                jnp.where(tall_ids == row[at:at + 1], val[g:g + 1], zero),
                jnp.where(tall_ids == col[at:at + 1], one, zero),
            )

        return hot

    def decode(start, totals):
        hots = [entries(start + i) for i in range(0, unit, batch)]
        sums = []
        for c in range(spans):
            left, right = zip(*(hot(c // per, c % per) for hot in hots))
            sums.append(
                totals[c] + mm_nt(jnp.concatenate(left, axis=1), jnp.concatenate(right, axis=1))
            )
        return sums

    for load in loads[-2:]:
        load.wait()
    sent = recv.at[pl.ds(0, devices - 1)]
    totals = [jnp.zeros((SPAN, SPAN), F32)] * spans
    for t in reversed(range(chips)):
        source = chip if t == chips - 1 else plane(t)
        first = source * nodes
        if t == 0:
            pltpu.make_async_copy(sent, sent, send_sem).wait()
        landed = recv.at[pl.ds(first, nodes - 1 if t == chips - 1 else nodes)]
        pltpu.make_async_copy(landed, landed, recv_sem.at[source]).wait()
        if unit == nodes:
            totals = decode(first, totals)
        else:
            totals = lax.fori_loop(
                0, nodes // unit, lambda i, old: decode(first + i * unit, old), totals
            )
    pairs = [jnp.concatenate(totals[c:c + 2], axis=1) for c in range(0, spans, 2)]
    chunk = max(1, len(pairs) // 2)
    for c in range(0, len(pairs), chunk):
        both = jnp.concatenate(halves(jnp.concatenate(pairs[c:c + chunk], axis=0)), axis=1)
        both = mm(both, right_cos[...])
        turned[c * SPAN:(c + chunk) * SPAN] = both[:, :LANES] + both[:, LANES:]
    power[...] = jnp.concatenate([jnp.sum(x * x, axis=0, keepdims=True) for x in pairs], axis=0)


def finish(new_in, turned, power, left_cos, new_hbm, upd_hbm, upd, sem):
    store_new = pltpu.make_async_copy(new_in, new_hbm.at[0], sem.at[0])
    store_new.start()
    strips = upd.shape[1] // (2 * LANES)
    pairs = power.shape[0]
    same = (
        lax.broadcasted_iota(jnp.int32, (LANES, LANES), 0) // SPAN
        == lax.broadcasted_iota(jnp.int32, (LANES, LANES), 1) // SPAN
    ).astype(F32).astype(BF16)
    energy = mm(jnp.concatenate(halves(power[...]), axis=0), same)
    energy = energy[:pairs] + energy[pairs:]
    scale = 1.0 / jnp.sqrt(energy * (1.0 / (SPAN * SPAN)) + 1.0)
    stores = [store_new]
    for c in range(0, pairs, 2):
        pieces = [turned[d * SPAN:(d + 1) * SPAN] for d in (c, c + 1)]
        high, low = halves(jnp.concatenate(pieces, axis=1))
        field = mm(left_cos[:, :3 * SPAN], jnp.concatenate([high, low, high], axis=0))
        level = jnp.concatenate([scale[c:c + 1], scale[c + 1:c + 2]], axis=1)
        a, s = c // 2 // strips, c // 2 % strips
        cut = pl.ds(a * SPAN, SPAN), pl.ds(s * 2 * LANES, 2 * LANES)
        upd[cut] = field * level
        store = pltpu.make_async_copy(upd.at[cut], upd_hbm.at[cut], sem.at[1 + c // 2])
        store.start()
        stores.append(store)
    for store in stores:
        store.wait()


def solution(mesh):
    nodes, chips = mesh.shape["node"], mesh.shape["chip"]

    def step(momentum, gradient, indices):
        _, rows, cols = momentum.shape
        spans, topk = indices.shape[1:]
        per = LANES // topk
        wide = per * SPAN
        used = 2 * (spans // per)
        tables = [jnp.asarray(x) for x in cosine_tables()]
        hbm = pl.BlockSpec(memory_space=pltpu.HBM)
        vmem = pl.BlockSpec(memory_space=pltpu.VMEM)
        operands = [momentum, gradient, indices, *tables]
        results = pl.pallas_call(
            functools.partial(kernel, nodes, chips, topk),
            out_shape=(
                pltpu.VMEM((rows, cols), F32),
                pltpu.VMEM((rows * cols // LANES, LANES), F32),
                pltpu.VMEM((spans // 2, LANES), F32),
                pltpu.VMEM(tables[2].shape, BF16),
            ),
            in_specs=[hbm] * 6,
            out_specs=(vmem,) * 4,
            scratch_shapes=[
                pltpu.VMEM(tables[1].shape, BF16),
                pltpu.VMEM(tables[0].shape, F32),
                pltpu.VMEM((rows, cols), F32),
                pltpu.VMEM((rows, cols), BF16),
                pltpu.VMEM((spans, topk), jnp.int32),
                pltpu.VMEM((used, LANES), BF16),
                pltpu.VMEM((nodes * chips, used, LANES), BF16),
                pltpu.SemaphoreType.DMA((6,)),
                pltpu.SemaphoreType.DMA,
                pltpu.SemaphoreType.DMA((chips,)),
            ],
            compiler_params=pltpu.CompilerParams(
                collective_id=0, has_side_effects=True, vmem_limit_bytes=24 * 2**20
            ),
        )(*(pltpu.with_memory_space_constraint(x, pltpu.HBM) for x in operands))
        return tuple(pl.pallas_call(
            finish,
            out_shape=(
                jax.ShapeDtypeStruct((1, rows, cols), F32),
                jax.ShapeDtypeStruct((rows, cols), F32),
            ),
            in_specs=[vmem] * 4,
            out_specs=(hbm, hbm),
            scratch_shapes=[
                pltpu.VMEM((rows, cols), F32),
                pltpu.SemaphoreType.DMA((1 + spans // 4,)),
            ],
            compiler_params=pltpu.CompilerParams(vmem_limit_bytes=24 * 2**20),
        )(*results))

    return jax.shard_map(
        step,
        mesh=mesh,
        in_specs=(P(("node", "chip"), None, None),) * 3,
        out_specs=(P(("node", "chip"), None, None), P()),
        check_vma=False,
    )
```

```python
import functools
import math

import jax
import jax.numpy as jnp
import numpy as np
from jax import lax
from jax.experimental import pallas as pl
from jax.experimental.pallas import tpu as pltpu
from jax.sharding import PartitionSpec as P

SPAN = 64
LANES = 128
MESH = pl.DeviceIdType.MESH
F32 = jnp.float32
BF16 = jnp.bfloat16


def cosine_tables():
    orders = np.arange(SPAN, dtype=np.float64)
    wave, cell = orders[:, None], orders[None, :]
    factor = np.where(wave == 0, math.sqrt(1 / SPAN), math.sqrt(2 / SPAN))
    table = factor * np.cos(math.pi * (2 * cell + 1) * wave / (2 * SPAN))
    high = table.astype(BF16)
    low = (table - high.astype(np.float64)).astype(BF16)
    pair = np.eye(LANES // SPAN, dtype=BF16)
    right = np.concatenate([np.kron(pair, high), np.kron(pair, low)], axis=1)
    left = np.concatenate([high.T, high.T, low.T, np.zeros_like(low)], axis=1)
    pick = np.pad(table.T, ((0, 0), (0, LANES - SPAN))).astype(F32)
    return pick, np.concatenate([right, right], axis=0), left


def halves(x):
    high = x.astype(BF16)
    return high, (x - high.astype(F32)).astype(BF16)


def mm(a, b):
    return lax.dot_general(a, b, (((1,), (0,)), ((), ())), preferred_element_type=F32)


def mm_nt(a, b):
    return lax.dot_general(a, b, (((1,), (1,)), ((), ())), preferred_element_type=F32)


def kernel(
    nodes, chips, topk, mom_hbm, grad_hbm, idx_hbm, pick_hbm, right_hbm, left_hbm, new_out, turned,
    power, left_cos, right_cos, pick, mom, grad, idx, box, recv, in_sem, send_sem, recv_sem,
):
    node, chip = lax.axis_index("node"), lax.axis_index("chip")
    devices = nodes * chips
    rows, cols = mom.shape
    per = LANES // topk
    wide = per * SPAN
    groups = idx.shape[0] // per
    strips = cols // wide
    batch = math.gcd(nodes, per)
    turn = node % batch

    bands = rows // SPAN
    loads = [
        (idx_hbm.at[0], idx),
        (pick_hbm, pick),
        (mom_hbm.at[0], mom),
        (grad_hbm.at[0], grad),
        (right_hbm, right_cos),
        (left_hbm, left_cos),
    ]
    loads = [pltpu.make_async_copy(*x, in_sem.at[i]) for i, x in enumerate(loads)]
    for load in loads[:2]:
        load.start()
    for src, dst, sem, priority, count in (
        (mom_hbm.at[0], mom, in_sem.at[2], 1, 8),
        (grad_hbm.at[0], grad, in_sem.at[3], 0, 4),
    ):
        for i in range(count):
            cut = pl.ds(i * rows // count, rows // count)
            pltpu.make_async_copy(src.at[cut], dst.at[cut], sem).start(priority=priority)

    barrier = pltpu.get_barrier_semaphore()

    unit = 2 * batch if nodes % (2 * batch) == 0 else batch
    high_side = 2 * chip >= chips

    def plane(t):
        up = t + (chip <= t).astype(jnp.int32)
        down = chips - 1 - t
        return jnp.where(high_side, up, down - (down <= chip).astype(jnp.int32))

    def peers(visit):
        def one(to_chip, i):
            @pl.when((to_chip != chip) | (i != node))
            def _():
                visit({"node": i, "chip": to_chip})

        for to_chip in range(chips):
            go = functools.partial(one, to_chip)
            if nodes <= 8:
                for i in range(nodes):
                    go(i)
            else:
                pl.loop(0, nodes)(go)

    def greet(to_chip, spot):
        pl.semaphore_signal(
            barrier, inc=1, device_id={"node": spot, "chip": to_chip}, device_id_type=MESH
        )

    def greet_own(i):
        spot = node + i
        greet(chip, jnp.where(spot >= nodes, spot - nodes, spot))

    for to_chip in map(plane, range(chips - 1)):
        if nodes <= 8:
            for spot in range(nodes):
                greet(to_chip, spot)
        else:
            pl.loop(0, nodes)(functools.partial(greet, to_chip))
    if nodes <= 8:
        for i in range(1, nodes):
            greet_own(i)
    else:
        pl.loop(1, nodes)(greet_own)

    loads[0].wait()
    slots = idx[...]
    spans = slots.shape[0]
    lane = lax.broadcasted_iota(jnp.int32, (spans, LANES), 1)
    place = lax.broadcasted_iota(jnp.int32, (spans, LANES), 0) % per
    spread = jnp.concatenate([slots] * per, axis=1)
    spread = jnp.where(lane // topk == (place + turn) % per, spread + place * (SPAN * SPAN), 0)
    lists = [
        jnp.sum(spread[g * per:(g + 1) * per], axis=0, keepdims=True) for g in range(groups)
    ]
    one, zero = jnp.ones((), BF16), jnp.zeros((), BF16)
    tall_ids = lax.broadcasted_iota(jnp.int32, (SPAN, LANES), 0).astype(F32).astype(BF16)
    wave = [((x // SPAN) % SPAN).astype(F32) for x in lists]
    cell = [(x % SPAN).astype(F32) for x in lists]
    loads[1].wait()

    def gather(row):
        spots = jnp.broadcast_to(row.astype(jnp.int32), (SPAN, LANES))
        return jnp.take_along_axis(pick[...], spots, axis=1, mode="promise_in_bounds")

    found = [halves(gather(x)) for x in cell]
    seat = (lax.broadcasted_iota(jnp.int32, (SPAN, LANES), 1) // topk + per - turn) % per

    def columns(x):
        return jnp.concatenate([jnp.where(seat == p, x, zero) for p in range(per)], axis=0)

    wide_high = [columns(x[0]) for x in found]
    wide_low = [columns(x[1]) for x in found]

    blended, picked = [], []
    for load in loads[2:-2]:
        load.wait()
    tall_cos = [gather(x) for x in wave]
    for a in range(bands):
        band = slice(a * SPAN, (a + 1) * SPAN)
        for b in range(strips):
            g = a * strips + b
            strip = slice(b * wide, (b + 1) * wide)
            blended.append(0.9 * mom[band, strip] + grad[band, strip].astype(F32))
            sums = mm(
                jnp.concatenate(halves(blended[g]), axis=0),
                jnp.concatenate([wide_high[g], wide_low[g]], axis=1),
            )
            sums = sums[:SPAN, :LANES] + (sums[SPAN:, :LANES] + sums[:SPAN, LANES:])
            picked.append(jnp.sum(sums * tall_cos[g], axis=0, keepdims=True))
    codes = [(1 + w / SPAN) * jnp.exp2(c - SPAN // 2) for w, c in zip(wave, cell)]
    payload = jnp.concatenate(picked + codes, axis=0).astype(BF16)
    me = chip * nodes + node
    box[...] = payload
    recv[me] = payload

    pl.semaphore_wait(barrier, devices - 1)
    peers(
        lambda to: pltpu.make_async_remote_copy(
            src_ref=box,
            dst_ref=recv.at[me],
            send_sem=send_sem,
            recv_sem=recv_sem.at[chip],
            device_id=to,
            device_id_type=MESH,
        ).start()
    )

    for load in loads[-2:]:
        load.start()

    for g in range(groups):
        sent_value = picked[g].astype(BF16).astype(F32)
        high, low = halves(tall_cos[g] * sent_value)
        own_part = mm_nt(high, wide_high[g]) + (
            mm_nt(low, wide_high[g]) + mm_nt(high, wide_low[g])
        )
        a, b = g // strips, g % strips
        new_out[a * SPAN:(a + 1) * SPAN, b * wide:(b + 1) * wide] = blended[g] - own_part

    part_row = lax.broadcasted_iota(jnp.int32, (2 * groups, LANES), 0)
    part_lane = lax.broadcasted_iota(jnp.int32, (2 * groups, LANES), 1) // topk
    empty = (part_row >= groups).astype(F32)

    def entries(start):
        rows = [recv[start + q].astype(F32) for q in range(batch)]
        hots = []
        for p in range(per):
            m = empty
            for q in range(batch):
                m = jnp.where(part_lane == (p + q) % per, rows[q], m)
            power = jnp.floor(jnp.log2(m) + 1 / SPAN / 4)
            col = (power + SPAN // 2).astype(BF16)
            row = jnp.floor((m * jnp.exp2(-power) - 1) * SPAN + 0.5).astype(BF16)
            hots.append((m.astype(BF16), row, col))

        def hot(g, p):
            val, row, col = hots[p]
            at = groups + g
            return (
                jnp.where(tall_ids == row[at:at + 1], val[g:g + 1], zero),
                jnp.where(tall_ids == col[at:at + 1], one, zero),
            )

        return hot

    def decode(start, totals):
        hots = [entries(start + i) for i in range(0, unit, batch)]
        sums = []
        for c in range(spans):
            left, right = zip(*(hot(c // per, c % per) for hot in hots))
            sums.append(
                totals[c] + mm_nt(jnp.concatenate(left, axis=1), jnp.concatenate(right, axis=1))
            )
        return sums

    for load in loads[-2:]:
        load.wait()
    sent = recv.at[pl.ds(0, devices - 1)]
    totals = [jnp.zeros((SPAN, SPAN), F32)] * spans
    for t in reversed(range(chips)):
        source = chip if t == chips - 1 else plane(t)
        first = source * nodes
        if t == 0:
            pltpu.make_async_copy(sent, sent, send_sem).wait()
        landed = recv.at[pl.ds(first, nodes - 1 if t == chips - 1 else nodes)]
        pltpu.make_async_copy(landed, landed, recv_sem.at[source]).wait()
        if unit == nodes:
            totals = decode(first, totals)
        else:
            totals = lax.fori_loop(
                0, nodes // unit, lambda i, old: decode(first + i * unit, old), totals
            )
    pairs = [jnp.concatenate(totals[c:c + 2], axis=1) for c in range(0, spans, 2)]
    chunk = max(1, len(pairs) // 2)
    for c in range(0, len(pairs), chunk):
        both = jnp.concatenate(halves(jnp.concatenate(pairs[c:c + chunk], axis=0)), axis=1)
        both = mm(both, right_cos[...])
        turned[c * SPAN:(c + chunk) * SPAN] = both[:, :LANES] + both[:, LANES:]
    power[...] = jnp.concatenate([jnp.sum(x * x, axis=0, keepdims=True) for x in pairs], axis=0)


def finish(new_in, turned, power, left_cos, new_hbm, upd_hbm, upd, sem):
    store_new = pltpu.make_async_copy(new_in, new_hbm.at[0], sem.at[0])
    store_new.start()
    strips = upd.shape[1] // (2 * LANES)
    pairs = power.shape[0]
    same = (
        lax.broadcasted_iota(jnp.int32, (LANES, LANES), 0) // SPAN
        == lax.broadcasted_iota(jnp.int32, (LANES, LANES), 1) // SPAN
    ).astype(F32).astype(BF16)
    energy = mm(jnp.concatenate(halves(power[...]), axis=0), same)
    energy = energy[:pairs] + energy[pairs:]
    scale = 1.0 / jnp.sqrt(energy * (1.0 / (SPAN * SPAN)) + 1.0)
    stores = [store_new]
    for c in range(0, pairs, 2):
        pieces = [turned[d * SPAN:(d + 1) * SPAN] for d in (c, c + 1)]
        high, low = halves(jnp.concatenate(pieces, axis=1))
        field = mm(left_cos[:, :3 * SPAN], jnp.concatenate([high, low, high], axis=0))
        level = jnp.concatenate([scale[c:c + 1], scale[c + 1:c + 2]], axis=1)
        a, s = c // 2 // strips, c // 2 % strips
        cut = pl.ds(a * SPAN, SPAN), pl.ds(s * 2 * LANES, 2 * LANES)
        upd[cut] = field * level
        store = pltpu.make_async_copy(upd.at[cut], upd_hbm.at[cut], sem.at[1 + c // 2])
        store.start()
        stores.append(store)
    for store in stores:
        store.wait()


def solution(mesh):
    nodes, chips = mesh.shape["node"], mesh.shape["chip"]

    def step(momentum, gradient, indices):
        _, rows, cols = momentum.shape
        spans, topk = indices.shape[1:]
        per = LANES // topk
        wide = per * SPAN
        used = 2 * (spans // per)
        tables = [jnp.asarray(x) for x in cosine_tables()]
        hbm = pl.BlockSpec(memory_space=pltpu.HBM)
        vmem = pl.BlockSpec(memory_space=pltpu.VMEM)
        operands = [momentum, gradient, indices, *tables]
        results = pl.pallas_call(
            functools.partial(kernel, nodes, chips, topk),
            out_shape=(
                pltpu.VMEM((rows, cols), F32),
                pltpu.VMEM((rows * cols // LANES, LANES), F32),
                pltpu.VMEM((spans // 2, LANES), F32),
                pltpu.VMEM(tables[2].shape, BF16),
            ),
            in_specs=[hbm] * 6,
            out_specs=(vmem,) * 4,
            scratch_shapes=[
                pltpu.VMEM(tables[1].shape, BF16),
                pltpu.VMEM(tables[0].shape, F32),
                pltpu.VMEM((rows, cols), F32),
                pltpu.VMEM((rows, cols), BF16),
                pltpu.VMEM((spans, topk), jnp.int32),
                pltpu.VMEM((used, LANES), BF16),
                pltpu.VMEM((nodes * chips, used, LANES), BF16),
                pltpu.SemaphoreType.DMA((6,)),
                pltpu.SemaphoreType.DMA,
                pltpu.SemaphoreType.DMA((chips,)),
            ],
            compiler_params=pltpu.CompilerParams(
                collective_id=0,
                has_side_effects=True,
                vmem_limit_bytes=24 * 2**20,
            ),
        )(*(pltpu.with_memory_space_constraint(x, pltpu.HBM) for x in operands))
        return tuple(pl.pallas_call(
            finish,
            out_shape=(
                jax.ShapeDtypeStruct((1, rows, cols), F32),
                jax.ShapeDtypeStruct((rows, cols), F32),
            ),
            in_specs=[vmem] * 4,
            out_specs=(hbm, hbm),
            scratch_shapes=[
                pltpu.VMEM((rows, cols), F32),
                pltpu.SemaphoreType.DMA((1 + spans // 4,)),
            ],
            compiler_params=pltpu.CompilerParams(vmem_limit_bytes=24 * 2**20),
        )(*results))

    return jax.shard_map(
        step,
        mesh=mesh,
        in_specs=(P(("node", "chip"), None, None),) * 3,
        out_specs=(P(("node", "chip"), None, None), P()),
        check_vma=False,
    )
```

```python
import functools
import math

import jax
import jax.numpy as jnp
import numpy as np
from jax import lax
from jax.experimental import pallas as pl
from jax.experimental.pallas import tpu as pltpu
from jax.sharding import PartitionSpec as P

SPAN = 64
LANES = 128
MESH = pl.DeviceIdType.MESH
F32 = jnp.float32
BF16 = jnp.bfloat16


def cosine_tables():
    orders = np.arange(SPAN, dtype=np.float64)
    wave, cell = orders[:, None], orders[None, :]
    factor = np.where(wave == 0, math.sqrt(1 / SPAN), math.sqrt(2 / SPAN))
    table = factor * np.cos(math.pi * (2 * cell + 1) * wave / (2 * SPAN))
    high = table.astype(BF16)
    low = (table - high.astype(np.float64)).astype(BF16)
    pair = np.eye(LANES // SPAN, dtype=BF16)
    right = np.concatenate([np.kron(pair, high), np.kron(pair, low)], axis=1)
    left = np.concatenate([high.T, high.T, low.T, np.zeros_like(low)], axis=1)
    pick = np.pad(table.T, ((0, 0), (0, LANES - SPAN))).astype(F32)
    return pick, np.concatenate([right, right], axis=0), left


def halves(x):
    high = x.astype(BF16)
    return high, (x - high.astype(F32)).astype(BF16)


def mm(a, b):
    return lax.dot_general(a, b, (((1,), (0,)), ((), ())), preferred_element_type=F32)


def mm_nt(a, b):
    return lax.dot_general(a, b, (((1,), (1,)), ((), ())), preferred_element_type=F32)


def kernel(
    nodes, chips, topk, mom_hbm, grad_hbm, idx_hbm, pick_hbm, right_hbm, left_hbm, new_out, turned,
    power, left_cos, right_cos, pick, mom, grad, idx, box, recv, in_sem, send_sem, recv_sem,
):
    node, chip = lax.axis_index("node"), lax.axis_index("chip")
    devices = nodes * chips
    rows, cols = mom.shape
    per = LANES // topk
    wide = per * SPAN
    groups = idx.shape[0] // per
    strips = cols // wide
    batch = math.gcd(nodes, per)
    turn = node % batch

    bands = rows // SPAN
    loads = [
        (idx_hbm.at[0], idx),
        (pick_hbm, pick),
        (mom_hbm.at[0], mom),
        (grad_hbm.at[0], grad),
        (right_hbm, right_cos),
        (left_hbm, left_cos),
    ]
    loads = [pltpu.make_async_copy(*x, in_sem.at[i]) for i, x in enumerate(loads)]
    loads[0].start()
    loads[1].start(priority=1)
    for src, dst, sem, priority, count in (
        (mom_hbm.at[0], mom, in_sem.at[2], 1, 8),
        (grad_hbm.at[0], grad, in_sem.at[3], 0, 4),
    ):
        for i in range(count):
            cut = pl.ds(i * rows // count, rows // count)
            pltpu.make_async_copy(src.at[cut], dst.at[cut], sem).start(priority=priority)

    barrier = pltpu.get_barrier_semaphore()

    unit = 2 * batch if nodes % (2 * batch) == 0 else batch
    high_side = 2 * chip >= chips

    def plane(t):
        up = t + (chip <= t).astype(jnp.int32)
        down = chips - 1 - t
        return jnp.where(high_side, up, down - (down <= chip).astype(jnp.int32))

    def peers(visit):
        def one(to_chip, i):
            @pl.when((to_chip != chip) | (i != node))
            def _():
                visit({"node": i, "chip": to_chip})

        for to_chip in range(chips):
            go = functools.partial(one, to_chip)
            if nodes <= 8:
                for i in range(nodes):
                    go(i)
            else:
                pl.loop(0, nodes)(go)

    def greet(to_chip, spot):
        pl.semaphore_signal(
            barrier, inc=1, device_id={"node": spot, "chip": to_chip}, device_id_type=MESH
        )

    def greet_own(i):
        spot = node + i
        greet(chip, jnp.where(spot >= nodes, spot - nodes, spot))

    for to_chip in map(plane, range(chips - 1)):
        if nodes <= 8:
            for spot in range(nodes):
                greet(to_chip, spot)
        else:
            pl.loop(0, nodes)(functools.partial(greet, to_chip))
    if nodes <= 8:
        for i in range(1, nodes):
            greet_own(i)
    else:
        pl.loop(1, nodes)(greet_own)

    loads[0].wait()
    slots = idx[...]
    spans = slots.shape[0]
    lane = lax.broadcasted_iota(jnp.int32, (spans, LANES), 1)
    place = lax.broadcasted_iota(jnp.int32, (spans, LANES), 0) % per
    spread = jnp.concatenate([slots] * per, axis=1)
    spread = jnp.where(lane // topk == (place + turn) % per, spread + place * (SPAN * SPAN), 0)
    lists = [
        jnp.sum(spread[g * per:(g + 1) * per], axis=0, keepdims=True) for g in range(groups)
    ]
    one, zero = jnp.ones((), BF16), jnp.zeros((), BF16)
    tall_ids = lax.broadcasted_iota(jnp.int32, (SPAN, LANES), 0).astype(F32).astype(BF16)
    wave = [((x // SPAN) % SPAN).astype(F32) for x in lists]
    cell = [(x % SPAN).astype(F32) for x in lists]
    loads[1].wait()

    def gather(row):
        spots = jnp.broadcast_to(row.astype(jnp.int32), (SPAN, LANES))
        return jnp.take_along_axis(pick[...], spots, axis=1, mode="promise_in_bounds")

    found = [halves(gather(x)) for x in cell]
    tall_cos = [gather(x) for x in wave]
    seat = (lax.broadcasted_iota(jnp.int32, (SPAN, LANES), 1) // topk + per - turn) % per

    def columns(x):
        return jnp.concatenate([jnp.where(seat == p, x, zero) for p in range(per)], axis=0)

    wide_high = [columns(x[0]) for x in found]
    wide_low = [columns(x[1]) for x in found]

    blended, picked = [], []
    for load in loads[2:-2]:
        load.wait()
    for a in range(bands):
        band = slice(a * SPAN, (a + 1) * SPAN)
        for b in range(strips):
            g = a * strips + b
            strip = slice(b * wide, (b + 1) * wide)
            blended.append(0.9 * mom[band, strip] + grad[band, strip].astype(F32))
            sums = mm(
                jnp.concatenate(halves(blended[g]), axis=0),
                jnp.concatenate([wide_high[g], wide_low[g]], axis=1),
            )
            sums = sums[:SPAN, :LANES] + (sums[SPAN:, :LANES] + sums[:SPAN, LANES:])
            picked.append(jnp.sum(sums * tall_cos[g], axis=0, keepdims=True))
    codes = [(1 + w / SPAN) * jnp.exp2(c - SPAN // 2) for w, c in zip(wave, cell)]
    payload = jnp.concatenate(picked + codes, axis=0).astype(BF16)
    me = chip * nodes + node
    box[...] = payload
    recv[me] = payload

    pl.semaphore_wait(barrier, devices - 1)
    peers(
        lambda to: pltpu.make_async_remote_copy(
            src_ref=box,
            dst_ref=recv.at[me],
            send_sem=send_sem,
            recv_sem=recv_sem.at[chip],
            device_id=to,
            device_id_type=MESH,
        ).start()
    )

    for load in loads[-2:]:
        load.start()

    for g in range(groups):
        sent_value = picked[g].astype(BF16).astype(F32)
        high, low = halves(tall_cos[g] * sent_value)
        own_part = mm_nt(high, wide_high[g]) + (
            mm_nt(low, wide_high[g]) + mm_nt(high, wide_low[g])
        )
        a, b = g // strips, g % strips
        new_out[a * SPAN:(a + 1) * SPAN, b * wide:(b + 1) * wide] = blended[g] - own_part

    part_row = lax.broadcasted_iota(jnp.int32, (2 * groups, LANES), 0)
    part_lane = lax.broadcasted_iota(jnp.int32, (2 * groups, LANES), 1) // topk
    empty = (part_row >= groups).astype(F32)

    def entries(start):
        rows = [recv[start + q].astype(F32) for q in range(batch)]
        hots = []
        for p in range(per):
            m = empty
            for q in range(batch):
                m = jnp.where(part_lane == (p + q) % per, rows[q], m)
            power = jnp.floor(jnp.log2(m) + 1 / SPAN / 4)
            col = (power + SPAN // 2).astype(BF16)
            row = jnp.floor((m * jnp.exp2(-power) - 1) * SPAN + 0.5).astype(BF16)
            hots.append((m.astype(BF16), row, col))

        def hot(g, p):
            val, row, col = hots[p]
            at = groups + g
            return (
                jnp.where(tall_ids == row[at:at + 1], val[g:g + 1], zero),
                jnp.where(tall_ids == col[at:at + 1], one, zero),
            )

        return hot

    def decode(start, totals):
        hots = [entries(start + i) for i in range(0, unit, batch)]
        sums = []
        for c in range(spans):
            left, right = zip(*(hot(c // per, c % per) for hot in hots))
            sums.append(
                totals[c] + mm_nt(jnp.concatenate(left, axis=1), jnp.concatenate(right, axis=1))
            )
        return sums

    for load in loads[-2:]:
        load.wait()
    sent = recv.at[pl.ds(0, devices - 1)]
    totals = [jnp.zeros((SPAN, SPAN), F32)] * spans
    for t in reversed(range(chips)):
        source = chip if t == chips - 1 else plane(t)
        first = source * nodes
        if t == 0:
            pltpu.make_async_copy(sent, sent, send_sem).wait()
        landed = recv.at[pl.ds(first, nodes - 1 if t == chips - 1 else nodes)]
        pltpu.make_async_copy(landed, landed, recv_sem.at[source]).wait()
        if unit == nodes:
            totals = decode(first, totals)
        else:
            totals = lax.fori_loop(
                0, nodes // unit, lambda i, old: decode(first + i * unit, old), totals
            )
    pairs = [jnp.concatenate(totals[c:c + 2], axis=1) for c in range(0, spans, 2)]
    chunk = max(1, len(pairs) // 2)
    for c in range(0, len(pairs), chunk):
        both = jnp.concatenate(halves(jnp.concatenate(pairs[c:c + chunk], axis=0)), axis=1)
        both = mm(both, right_cos[...])
        turned[c * SPAN:(c + chunk) * SPAN] = both[:, :LANES] + both[:, LANES:]
    power[...] = jnp.concatenate([jnp.sum(x * x, axis=0, keepdims=True) for x in pairs], axis=0)


def finish(new_in, turned, power, left_cos, new_hbm, upd_hbm, upd, sem):
    store_new = pltpu.make_async_copy(new_in, new_hbm.at[0], sem.at[0])
    store_new.start()
    strips = upd.shape[1] // (2 * LANES)
    pairs = power.shape[0]
    same = (
        lax.broadcasted_iota(jnp.int32, (LANES, LANES), 0) // SPAN
        == lax.broadcasted_iota(jnp.int32, (LANES, LANES), 1) // SPAN
    ).astype(F32).astype(BF16)
    energy = mm(jnp.concatenate(halves(power[...]), axis=0), same)
    energy = energy[:pairs] + energy[pairs:]
    scale = 1.0 / jnp.sqrt(energy * (1.0 / (SPAN * SPAN)) + 1.0)
    stores = [store_new]
    for c in range(0, pairs, 2):
        pieces = [turned[d * SPAN:(d + 1) * SPAN] for d in (c, c + 1)]
        high, low = halves(jnp.concatenate(pieces, axis=1))
        field = mm(left_cos[:, :3 * SPAN], jnp.concatenate([high, low, high], axis=0))
        level = jnp.concatenate([scale[c:c + 1], scale[c + 1:c + 2]], axis=1)
        a, s = c // 2 // strips, c // 2 % strips
        cut = pl.ds(a * SPAN, SPAN), pl.ds(s * 2 * LANES, 2 * LANES)
        upd[cut] = field * level
        store = pltpu.make_async_copy(upd.at[cut], upd_hbm.at[cut], sem.at[1 + c // 2])
        store.start()
        stores.append(store)
    for store in stores:
        store.wait()


def solution(mesh):
    nodes, chips = mesh.shape["node"], mesh.shape["chip"]

    def step(momentum, gradient, indices):
        _, rows, cols = momentum.shape
        spans, topk = indices.shape[1:]
        per = LANES // topk
        wide = per * SPAN
        used = 2 * (spans // per)
        tables = [jnp.asarray(x) for x in cosine_tables()]
        hbm = pl.BlockSpec(memory_space=pltpu.HBM)
        vmem = pl.BlockSpec(memory_space=pltpu.VMEM)
        operands = [momentum, gradient, indices, *tables]
        results = pl.pallas_call(
            functools.partial(kernel, nodes, chips, topk),
            out_shape=(
                pltpu.VMEM((rows, cols), F32),
                pltpu.VMEM((rows * cols // LANES, LANES), F32),
                pltpu.VMEM((spans // 2, LANES), F32),
                pltpu.VMEM(tables[2].shape, BF16),
            ),
            in_specs=[hbm] * 6,
            out_specs=(vmem,) * 4,
            scratch_shapes=[
                pltpu.VMEM(tables[1].shape, BF16),
                pltpu.VMEM(tables[0].shape, F32),
                pltpu.VMEM((rows, cols), F32),
                pltpu.VMEM((rows, cols), BF16),
                pltpu.VMEM((spans, topk), jnp.int32),
                pltpu.VMEM((used, LANES), BF16),
                pltpu.VMEM((nodes * chips, used, LANES), BF16),
                pltpu.SemaphoreType.DMA((6,)),
                pltpu.SemaphoreType.DMA,
                pltpu.SemaphoreType.DMA((chips,)),
            ],
            compiler_params=pltpu.CompilerParams(
                collective_id=0,
                has_side_effects=True,
                vmem_limit_bytes=24 * 2**20,
            ),
        )(*(pltpu.with_memory_space_constraint(x, pltpu.HBM) for x in operands))
        return tuple(pl.pallas_call(
            finish,
            out_shape=(
                jax.ShapeDtypeStruct((1, rows, cols), F32),
                jax.ShapeDtypeStruct((rows, cols), F32),
            ),
            in_specs=[vmem] * 4,
            out_specs=(hbm, hbm),
            scratch_shapes=[
                pltpu.VMEM((rows, cols), F32),
                pltpu.SemaphoreType.DMA((1 + spans // 4,)),
            ],
            compiler_params=pltpu.CompilerParams(vmem_limit_bytes=24 * 2**20),
        )(*results))

    return jax.shard_map(
        step,
        mesh=mesh,
        in_specs=(P(("node", "chip"), None, None),) * 3,
        out_specs=(P(("node", "chip"), None, None), P()),
        check_vma=False,
    )
```
